32 devices in a mesh: row: 8 (over z, y), col: 4 (over x, core).
Axes of the slice: x: 2, y: 2, z: 4, core: 2. Of those that a mesh axis runs over, the one named last changes fastest.
Arguments:
- matrix: bfloat16 [32768, 32768], P('row', 'col'), may hold values from -0.03125 to 0.03125
- right_sides: float32 [32768, 64], P(('row', 'col')), may hold values from -6 to 6
- initial_guess: float32 [32768, 64], P(('row', 'col')), may hold values from -6 to 6
Outputs:
- solution: float32 [32768, 64], P(('row', 'col'))
The draws below stay inside these ranges and needn't reach their ends.
All inputs are finite; a program needn't handle non-finite values.
Results may differ from the reference program's by a relative error of at most 0.0038.
Values may be sent and summed in bfloat16 or wider, within the bound.
No kernel may reach another device: no remote copies, remote signals or barrier semaphores. Data moves between devices by JAX's collectives and lax.ppermute only.
A program may use at most 128 MiB of HBM per device.

```python
import jax
import jax.numpy as jnp
from jax import lax

N = 32768
S = 64
STEPS = 3
PROW = 8
PCOL = 4
CH = 1024


def steps_of(stream_key, extent, cuts, least, high):
    factor_of, own = 1.0, jax.random.fold_in(stream_key, 6)
    for axis_at, parts in cuts:
        heights = jnp.exp(jax.random.uniform(jax.random.fold_in(own, axis_at), (parts,), jnp.float32, least / len(cuts), high / len(cuts)))
        factor_of = factor_of * jnp.repeat(heights, extent[axis_at] // parts).reshape([-1 if axis == axis_at else 1 for axis in range(len(extent))])
    return factor_of


def scatter_about(key, extent, scale, most, cuts=(), kind=jnp.bfloat16):
    factor_of = steps_of(key, extent, cuts, -0.22, 0.18) if cuts else 1.0
    values = jax.random.normal(key, extent, jnp.float32) * scale * factor_of
    return jnp.minimum(jnp.maximum(values, -most), most).astype(kind)


def setup_inputs(seed: int = 0) -> dict:
    splits = jax.random.split(jax.random.key(seed), 4)
    return {
        "matrix": scatter_about(splits[0], (N, N), N ** -0.5, 0.03125, ((0, 8), (1, 4))),
        "right_sides": scatter_about(splits[1], (N, S), 1.0, 6.0, ((0, 32),), jnp.float32),
        "initial_guess": scatter_about(splits[2], (N, S), 1.0, 6.0, ((0, 32),), jnp.float32),
    }


DIAGONAL_SHIFT = 1.4

def inner_products(left, right):
    return jnp.einsum('rk,rs->ks', left, right, precision=lax.Precision.HIGHEST)

def combine_basis(stacked, weights):
    return jnp.dot(stacked, weights, precision=lax.Precision.HIGHEST)

def orthonormal(applied, gram_sum):
    lower_factor = jnp.linalg.cholesky(gram_sum)
    basis_next = lax.linalg.triangular_solve(lower_factor, applied, left_side=False, lower=True, transpose_a=True)
    return (basis_next, lower_factor.T)

def least_squares(column_list, top_factor):
    span_width = top_factor.shape[0]
    count = len(column_list)
    pieces = []
    for position, (projected, upper_factor) in enumerate(column_list):
        filler = jnp.zeros(((count - position - 1) * span_width, span_width), jnp.float32)
        pieces.append(jnp.concatenate([projected, upper_factor, filler], axis=0))
    hessenberg = jnp.concatenate(pieces, axis=1)
    normal_matrix = inner_products(hessenberg, hessenberg)
    target = inner_products(hessenberg[:span_width], top_factor)
    lower_factor = jnp.linalg.cholesky(normal_matrix)
    halfway = lax.linalg.triangular_solve(lower_factor, target, left_side=True, lower=True)
    return lax.linalg.triangular_solve(lower_factor, halfway, left_side=True, lower=True, transpose_a=True)

def operate(block_now, matrix):
    rounded = lax.optimization_barrier(block_now.astype(jnp.bfloat16))
    ordered = rounded.reshape(PROW, PCOL, CH, S).transpose(1, 0, 2, 3).reshape(N, S).astype(jnp.float32)

    def row_panel(panel_rows):
        return jnp.dot(panel_rows.astype(jnp.float32), ordered, precision=lax.Precision.HIGHEST)
    product = lax.map(row_panel, matrix.reshape(PROW, N // PROW, N)).reshape(N, S)
    return DIAGONAL_SHIFT * block_now + product

def reference(matrix, right_sides, initial_guess):
    residual_start = right_sides - operate(initial_guess, matrix)
    basis_now, top_factor = orthonormal(residual_start, inner_products(residual_start, residual_start))
    basis_list = [basis_now]
    column_list = []
    for iteration in range(STEPS):
        applied = operate(basis_list[-1], matrix)
        stacked = jnp.concatenate(basis_list, axis=1)
        projected = inner_products(stacked, applied)
        applied = applied - combine_basis(stacked, projected)
        gram_sum = inner_products(applied, applied)
        basis_now, upper_factor = orthonormal(applied, gram_sum)
        basis_list.append(basis_now)
        column_list.append((projected, upper_factor))
    coefficients = least_squares(column_list, top_factor)
    update = combine_basis(jnp.concatenate(basis_list[:-1], axis=1), coefficients)
    return initial_guess + update
```

```python
import functools

import jax
import jax.numpy as jnp
from jax import lax
from jax.experimental import pallas as pl
from jax.experimental.pallas import tpu as pltpu
from jax.sharding import PartitionSpec as P

STEPS = 3


DIAGONAL_SHIFT = 1.4


def dot_rows(left, right):
    return lax.dot_general(
        left, right, (((1,), (1,)), ((), ())), precision=lax.Precision.HIGHEST
    )


def matmul(left, right):
    return jnp.dot(left, right, precision=lax.Precision.HIGHEST)


def invert_lower(lower_factor):
    identity = jnp.eye(lower_factor.shape[0], dtype=lower_factor.dtype)
    return lax.linalg.triangular_solve(lower_factor, identity, left_side=True, lower=True)


def panel_kernel(place, matrix, piece, *refs):
    product = lax.dot_general(
        piece[...], matrix[...], (((1,), (1,)), ((), ())), preferred_element_type=jnp.float32
    )
    if len(refs) == 2:
        product = refs[0][...] + product
    refs[-1][...] = product


def panel_product(matrix, piece, place, total, first, blocks, stride, chunk):
    span, width = piece.shape

    def row_block(step, place_ref):
        position = step + first
        other = 1 - position // stride
        parity = (place_ref[1] + other) % 2
        return 2 * (position % stride) + parity

    specs = [
        pl.BlockSpec((chunk, width), lambda step, ref: (row_block(step, ref), ref[0])),
        pl.BlockSpec((span, width), lambda step, ref: (0, 0)),
    ]
    operands = [matrix, piece]
    if total is not None:
        specs.append(pl.BlockSpec((span, chunk), lambda step, ref: (0, step + first)))
        operands.append(total)
    return pl.pallas_call(
        panel_kernel,
        out_shape=jax.ShapeDtypeStruct((span, blocks * chunk), jnp.float32),
        grid_spec=pltpu.PrefetchScalarGridSpec(
            num_scalar_prefetch=1,
            grid=(blocks,),
            in_specs=specs,
            out_specs=pl.BlockSpec((span, chunk), lambda step, ref: (0, step)),
        ),
        compiler_params=pltpu.CompilerParams(dimension_semantics=("arbitrary",)),
    )(place, *operands)


def per_device(matrix, right_sides, initial_guess, rows, cols):
    row_at = lax.axis_index("row")
    col_at = lax.axis_index("col")
    chunk = initial_guess.shape[0]
    nodes, half = rows // 2, cols // 2
    node_at, x_at, parity = row_at // 2, col_at // 2, col_at % 2

    def ring(block, shift):
        pairs = [(i, (i + 2 * shift) % rows) for i in range(rows)]
        return lax.ppermute(block, "row", pairs)

    def place_of(node):
        return jnp.stack([node % nodes, parity]).astype(jnp.int32)

    def product_of(block):
        operand = block.astype(jnp.bfloat16)
        mate = lax.ppermute(operand, "row", [(i, i ^ 1) for i in range(rows)])
        first = row_at % 2 == 0
        pair = jnp.concatenate(
            [jnp.where(first, operand, mate), jnp.where(first, mate, operand)], axis=1
        )
        forward = backward = pair
        queue = [(pair, node_at)]
        for hop in range(1, nodes // 2 + 1):
            forward = ring(forward, 1)
            queue.append((forward, node_at - hop + nodes))
            if 2 * hop != nodes:
                backward = ring(backward, -1)
                queue.append((backward, node_at + hop))
        total = None
        multiply = functools.partial(panel_product, matrix, stride=half, chunk=chunk)
        for piece, node in queue[:-1]:
            total = multiply(piece, place_of(node), total, first=0, blocks=cols)
        piece, node = queue[-1]
        away = multiply(piece, place_of(node), total, first=0, blocks=half)
        arrived = lax.ppermute(away, "col", [(i, i ^ 1) for i in range(cols)])
        kept = multiply(piece, place_of(node), total, first=half, blocks=half)
        summed = kept + arrived

        def block_of(at):
            return lax.dynamic_slice_in_dim(summed, at * chunk, chunk, axis=1)

        result = block_of(x_at)
        for shift in range(1, half):
            pairs = [(i, (i + 2 * shift) % cols) for i in range(cols)]
            result = result + lax.ppermute(block_of((x_at + shift) % half), "col", pairs)
        return result

    def operate(block):
        return DIAGONAL_SHIFT * block + product_of(block)

    def reduce_all(local_sum):
        for axis, count in (("col", cols), ("row", rows)):
            bit = 1
            while bit < count:
                pairs = [(i, i ^ bit) for i in range(count)]
                local_sum = local_sum + lax.ppermute(local_sum, axis, pairs)
                bit *= 2
        return local_sum

    guess, sides = initial_guess.T, right_sides.T
    span = guess.shape[0]
    residual = sides - operate(guess)
    lower_start = jnp.linalg.cholesky(reduce_all(dot_rows(residual, residual)))
    basis = matmul(invert_lower(lower_start), residual)
    stacked = basis
    columns, normal, factor, sides_small = [], {}, {}, []
    inverses, halfway = [], []
    for step in range(STEPS):
        applied = operate(basis)
        everything = jnp.concatenate([stacked, applied], axis=0)
        combined = reduce_all(dot_rows(applied, everything))
        width = stacked.shape[0]
        projected, own = combined[:, :width], combined[:, width:]
        row = [matmul(projected[:, : before.shape[1]], before.T) for before in columns] + [own]
        target = dot_rows(projected[:, :span], lower_start)
        for at, block in enumerate(row):
            for earlier in range(at):
                block = block - dot_rows(factor[step, earlier], factor[at, earlier])
            if at < step:
                factor[step, at] = dot_rows(block, inverses[at])
            else:
                inverses.append(invert_lower(jnp.linalg.cholesky(block)))
        for earlier in range(step):
            target = target - matmul(factor[step, earlier], halfway[earlier])
        halfway.append(matmul(inverses[step], target))
        if step + 1 == STEPS:
            break
        lower = jnp.linalg.cholesky(own - dot_rows(projected, projected))
        cleaned = applied - matmul(projected, stacked)
        basis = matmul(invert_lower(lower), cleaned)
        stacked = jnp.concatenate([stacked, basis], axis=0)
        columns.append(jnp.concatenate([projected, lower], axis=1))
    answers = [None] * STEPS
    for at in reversed(range(STEPS)):
        block = halfway[at]
        for later in range(at + 1, STEPS):
            block = block - matmul(factor[later, at].T, answers[later])
        answers[at] = matmul(inverses[at].T, block)
    coefficients = jnp.concatenate(answers, axis=0)
    update = matmul(coefficients.T, stacked)
    return (guess + update).T


def solution(mesh):
    return jax.shard_map(
        functools.partial(per_device, rows=mesh.shape["row"], cols=mesh.shape["col"]),
        mesh=mesh,
        in_specs=(P("row", "col"), P(("row", "col"), None), P(("row", "col"), None)),
        out_specs=P(("row", "col"), None),
        check_vma=False,
    )
```
